16 devices in a mesh: rep: 1, dp: 16 (over x, y, z, core).
Axes of the slice: x: 2, y: 2, z: 2, core: 2. Of those that a mesh axis runs over, the one named last changes fastest.
Arguments:
- x: bfloat16 [16, 2048, 1024], P(('rep', 'dp'))
- dy: bfloat16 [16, 2048, 1024], P(('rep', 'dp'))
- wq: bfloat16 [2, 1024, 1536], P(None, 'dp')
- wk: bfloat16 [2, 1024, 256], P(None, 'dp')
- wv: bfloat16 [2, 1024, 256], P(None, 'dp')
- wo: bfloat16 [2, 1536, 1024], P(None, 'dp')
- w_gate: bfloat16 [2, 1024, 4096], P(None, 'dp')
- w_up: bfloat16 [2, 1024, 4096], P(None, 'dp')
- w_down: bfloat16 [2, 4096, 1024], P(None, 'dp')
Outputs:
- output 1: bfloat16 [16, 2048, 1024], P(('rep', 'dp'))
- output 2: bfloat16 [2, 1024, 1536], P('rep', 'dp')
- output 3: bfloat16 [2, 1024, 256], P('rep', 'dp')
- output 4: bfloat16 [2, 1024, 256], P('rep', 'dp')
- output 5: bfloat16 [2, 1536, 1024], P('rep', 'dp')
- output 6: bfloat16 [2, 1024, 4096], P('rep', 'dp')
- output 7: bfloat16 [2, 1024, 4096], P('rep', 'dp')
- output 8: bfloat16 [2, 4096, 1024], P('rep', 'dp')
All inputs are finite; a program needn't handle non-finite values.
Results may differ from the reference program's by a relative error of at most 0.0312.
Values are sent between devices in bfloat16 or wider.
A program may use at most 2 GiB of HBM per device.

```python
import jax
import jax.numpy as jnp
from jax import lax

SEQUENCES = 16
TOKENS = 2048
D = 1024
HEADS = 12
KV_HEADS = 2
HEAD = 128
FF = 4096
LAYERS = 2
THETA = 10000
NAMES = ("wq", "wk", "wv", "wo", "w_gate", "w_up", "w_down")
SHAPES = {
    "wq": (LAYERS, D, HEADS * HEAD),
    "wk": (LAYERS, D, KV_HEADS * HEAD),
    "wv": (LAYERS, D, KV_HEADS * HEAD),
    "wo": (LAYERS, HEADS * HEAD, D),
    "w_gate": (LAYERS, D, FF),
    "w_up": (LAYERS, D, FF),
    "w_down": (LAYERS, FF, D),
}


def bump(key, n, height):
    away = (jnp.arange(n, dtype=jnp.int32) - jax.random.randint(key, (), 0, n, jnp.int32)) % n
    return jnp.where(away < n // 8, height, 1.0)


def together(key, own, strength):
    shared = jax.random.normal(key, own.shape[1:], jnp.float32)
    return (own + strength * shared) * lax.rsqrt(1 + strength * strength)


def setup_inputs(seed: int = 0, part: int = 0) -> dict:
    kx, kdy, ka, kb, kz, kf, kh, kl, *keys = jax.random.split(jax.random.key(seed), 8 + 3 * len(NAMES))
    kx, kdy, ka, kb = (jax.random.fold_in(k, part) for k in (kx, kdy, ka, kb))
    kw, km, kv = (keys[i::3] for i in range(3))
    shape = (SEQUENCES, TOKENS, D)
    much_x, much_dy = jax.random.uniform(kz, (2,), jnp.float32, 0.0, 1.0)
    loud = 2.0 ** jax.random.uniform(jax.random.fold_in(kz, 1), (), jnp.float32, -1.0, 2.0)
    layers = 2.0 ** jax.random.uniform(kl, (LAYERS, 1, 1), jnp.float32, -1.0, 1.0)
    times = {"wq": 1.0, "wk": 1.0, "wv": 2.0, "wo": layers, "w_gate": 1.0, "w_up": bump(kh, FF, 4.0), "w_down": layers}
    x = together(ka, jax.random.normal(kx, shape, jnp.float32), much_x) * bump(kf, D, 4.0)
    dy = together(kb, jax.random.normal(kdy, shape, jnp.float32), much_dy)
    drawn = {"x": x.astype(jnp.bfloat16), "dy": (loud * dy * (SEQUENCES * TOKENS) ** -0.5).astype(jnp.bfloat16)}
    for key, name in zip(kw, NAMES, strict=True):
        drawn[name] = (jax.random.normal(key, SHAPES[name], jnp.float32) * SHAPES[name][1] ** -0.5 * times[name]).astype(jnp.bfloat16)
    return drawn


def matmul(a, w):
    return jnp.dot(a, w, preferred_element_type=jnp.float32).astype(jnp.bfloat16)


def normed(h):
    wide = h.astype(jnp.float32)
    scale = lax.rsqrt(jnp.mean(wide**2, -1, keepdims=True) + 1e-6)
    return (wide * scale).astype(jnp.bfloat16)


def turned(t, theta):
    half = t.shape[-1] // 2
    angle = jnp.arange(t.shape[0], dtype=jnp.float32)[:, None] * theta ** (-jnp.arange(half, dtype=jnp.float32) / half)
    cos, sin = jnp.cos(angle)[:, None], jnp.sin(angle)[:, None]
    a, b = t[..., :half].astype(jnp.float32), t[..., half:].astype(jnp.float32)
    return jnp.concatenate([a * cos - b * sin, b * cos + a * sin], -1).astype(jnp.bfloat16)


def seen_by(q, k, v):
    tokens, kv = q.shape[0], k.shape[1]
    q = q.reshape(tokens, kv, -1, q.shape[-1])
    scores = jnp.einsum("tgsd,ugd->gstu", q.astype(jnp.float32), k.astype(jnp.float32)) * q.shape[-1] ** -0.5
    place = jnp.arange(tokens)
    weights = jax.nn.softmax(jnp.where(place[:, None] >= place, scores, -jnp.inf), -1).astype(jnp.bfloat16)
    return jnp.einsum("gstu,ugd->tgsd", weights.astype(jnp.float32), v.astype(jnp.float32)).astype(jnp.bfloat16).reshape(tokens, -1)


def layer(h, w):
    a = normed(h)
    q, k = (turned(matmul(a, w[name]).reshape(h.shape[0], -1, HEAD), THETA) for name in ("wq", "wk"))
    h = h + matmul(seen_by(q, k, matmul(a, w["wv"]).reshape(h.shape[0], -1, HEAD)), w["wo"])
    b = normed(h)
    gate = jnp.dot(b, w["w_gate"], preferred_element_type=jnp.float32)
    up = jnp.dot(b, w["w_up"], preferred_element_type=jnp.float32)
    return h + matmul((jax.nn.silu(gate) * up).astype(jnp.bfloat16), w["w_down"])


def stack(weights, h):
    return lax.scan(lambda h, w: (layer(h, w), None), h, weights)[0]


def reference(x, dy, wq, wk, wv, wo, w_gate, w_up, w_down):
    weights = dict(zip(NAMES, (wq, wk, wv, wo, w_gate, w_up, w_down), strict=True))

    def take(so_far, sequence):
        h, by_y = sequence
        _, back = jax.vjp(stack, weights, h)
        by_weights, by_h = back(by_y)
        return jax.tree.map(lambda total, term: total + term.astype(jnp.float32), so_far, by_weights), by_h

    none_yet = {name: jnp.zeros(w.shape, jnp.float32) for name, w in weights.items()}
    by_weights, by_x = lax.scan(take, none_yet, (x, dy))
    return (by_x, *(by_weights[name].astype(jnp.bfloat16) for name in NAMES))
```

```python
import functools

import jax
import jax.numpy as jnp
from jax import lax
from jax.experimental import pallas as pl
from jax.experimental.pallas import tpu as pltpu
from jax.sharding import PartitionSpec as P

NEG = -1e30
HIDDEN = 2 * NEG
LOG2E = 1.4426950408889634
HEAD = 128
HEADS = 12
KV = 2
GROUP = HEADS // KV
QW = HEADS * HEAD
KW = KV * HEAD
THETA = 10000
BF = jnp.bfloat16
F32 = jnp.float32
NAMES = ("wq", "wk", "wv", "wo", "w_gate", "w_up", "w_down")


def _dot(a, b, ca, cb):
    return lax.dot_general(a, b, (((ca,), (cb,)), ((), ())), preferred_element_type=F32)


def _params(steps=1, mib=60):
    return pltpu.CompilerParams(dimension_semantics=("arbitrary",) * steps, vmem_limit_bytes=mib * 2**20)


def _cost(flops, arrays, exps=0):
    return pl.CostEstimate(flops=int(flops), transcendentals=int(exps), bytes_accessed=sum(a.size * a.dtype.itemsize for a in arrays))


def _whole(*shape, once=False):
    mode = dict(pipeline_mode=pl.Buffered(1)) if once else {}
    return pl.BlockSpec(shape, lambda *_: (0,) * len(shape), **mode)


def _shape(*shape, dtype=BF):
    return jax.ShapeDtypeStruct(shape, dtype)


def _turn(t, cos, sin):
    return t * cos + pltpu.roll(t, HEAD // 2, 1) * sin


def _turn_back(t, cos, sin):
    return t * cos - pltpu.roll(t, HEAD // 2, 1) * sin


def tables(tokens):
    half = HEAD // 2
    angle = jnp.arange(tokens, dtype=F32)[:, None] * THETA ** (-jnp.arange(half, dtype=F32) / half)
    cos, sin = jnp.cos(angle), jnp.sin(angle)
    return jnp.concatenate([cos, cos], 1), jnp.concatenate([-sin, sin], 1)


def _gap(bk, cols, bq):
    return lax.rem(lax.broadcasted_iota(jnp.int32, (bk, cols), 1), bq) - lax.broadcasted_iota(jnp.int32, (bk, cols), 0)


def _attend(q_ref, k_ref, v_ref, cos_ref, sin_ref, o_ref, lse_ref, q_s, k_s, v_s, top_s, mix_s, gap_s, *, bq, wide, big, small):
    tokens = k_ref.shape[0]
    cols = GROUP * bq
    iq = pl.program_id(0)
    scale = HEAD**-0.5
    e = scale * LOG2E
    pieces = [(i, at) for i in range(KV) for at in range(0, cols, wide)]

    @pl.when(iq == 0)
    def _():
        gap_s[...] = _gap(small, cols, bq)
        chunk = 256

        def prepare(n, _):
            rows = pl.ds(pl.multiple_of(n * chunk, chunk), chunk)
            cos, sin = cos_ref[rows, :], sin_ref[rows, :]
            for i in range(KV):
                at = slice(i * HEAD, (i + 1) * HEAD)
                k_s[i, rows, :] = _turn(k_ref[rows, at].astype(F32), cos, sin).astype(BF)
                v_s[i, :HEAD, rows] = v_ref[rows, at].astype(F32).T.astype(BF)
                v_s[i, HEAD:, rows] = jnp.ones((16, chunk), BF)
            return _

        lax.fori_loop(0, tokens // chunk, prepare, None)

    mine = pl.ds(pl.multiple_of(iq * bq, bq), bq)
    cos, sin = cos_ref[mine, :], sin_ref[mine, :]
    for i in range(KV):
        for n in range(GROUP):
            at = (i * GROUP + n) * HEAD
            q_s[i, n * bq : (n + 1) * bq, :] = _turn(q_ref[:, at : at + HEAD].astype(F32), cos, sin).astype(BF)
    top_s[...] = jnp.full(top_s.shape, NEG, F32)
    mix_s[...] = jnp.zeros(mix_s.shape, F32)

    def block(start, size, masked):
        here = pl.ds(pl.multiple_of(start, small), size)
        scores = [_dot(k_s[i, here, :], q_s[i, at : at + wide, :], 1, 1) for i, at in pieces]
        weights, keeps = [], []
        level = start - iq * bq
        for (i, at), s in zip(pieces, scores):
            if masked:
                s = jnp.where(gap_s[:, at : at + wide] >= level, s, HIDDEN)
            old = top_s[i : i + 1, at : at + wide]
            top = jnp.maximum(old, s.max(axis=0, keepdims=True))
            top_s[i : i + 1, at : at + wide] = top
            weights.append(jnp.exp2((s - top) * e).astype(BF))
            keeps.append(jnp.exp2((old - top) * e))
        for (i, at), p, keep in zip(pieces, weights, keeps):
            mix_s[i, :, at : at + wide] = mix_s[i, :, at : at + wide] * keep + _dot(v_s[i, :, here], p, 1, 0)

    first = iq * bq
    lax.fori_loop(0, lax.div(first, big), lambda j, _: block(j * big, big, False), None)
    lax.fori_loop(lax.div(first, big) * (big // small), lax.div(first + bq + small - 1, small), lambda j, _: block(j * small, small, True), None)

    for i in range(KV):
        top, total = top_s[i : i + 1, :], mix_s[i, HEAD : HEAD + 1, :]
        out = (mix_s[i, :HEAD, :] * (1 / total)).T
        lse = top * scale + jnp.log(total)
        for n in range(GROUP):
            at = (i * GROUP + n) * HEAD
            o_ref[:, at : at + HEAD] = out[n * bq : (n + 1) * bq, :].astype(BF)
            lse_ref[i, n : n + 1, :] = lse[:, n * bq : (n + 1) * bq]


def attend(qkv, cos, sin, bq=256, wide=512, big=512, small=256):
    tokens = qkv.shape[0]
    cols = GROUP * bq
    return pl.pallas_call(
        functools.partial(_attend, bq=bq, wide=wide, big=big, small=small),
        grid=(tokens // bq,),
        in_specs=[pl.BlockSpec((bq, QW), lambda i: (i, 0)), pl.BlockSpec((tokens, KW), lambda i: (0, QW // KW)),
                  pl.BlockSpec((tokens, KW), lambda i: (0, QW // KW + 1)), _whole(tokens, HEAD), _whole(tokens, HEAD)],
        out_specs=[pl.BlockSpec((bq, QW), lambda i: (i, 0)), pl.BlockSpec((KV, GROUP, bq), lambda i: (0, 0, i))],
        out_shape=[_shape(tokens, QW), _shape(KV, GROUP, tokens, dtype=F32)],
        scratch_shapes=[pltpu.VMEM((KV, cols, HEAD), BF), pltpu.VMEM((KV, tokens, HEAD), BF), pltpu.VMEM((KV, HEAD + 16, tokens), BF),
                        pltpu.VMEM((KV, cols), F32), pltpu.VMEM((KV, HEAD + 16, cols), F32), pltpu.VMEM((small, cols), jnp.int32)],
        compiler_params=_params(),
        cost_estimate=_cost(2 * HEADS * tokens * tokens * HEAD, [qkv, qkv], HEADS * tokens * tokens // 2),
        name="attend",
    )(qkv, qkv, qkv, cos, sin)


def _attend_back(q_ref, k_ref, v_ref, o_ref, do_ref, lse_ref, cos_ref, sin_ref, d_ref, q_s, do_s, k_s, kt_s, v_s, dq_s, dk_s, dv_s, stat_s, gap_s,
                 *, bq, wide, big, small):
    tokens = k_ref.shape[0]
    cols = GROUP * bq
    iq = pl.program_id(0)
    scale = HEAD**-0.5
    e = scale * LOG2E
    pieces = [(i, at) for i in range(KV) for at in range(0, cols, wide)]
    chunk = 256

    @pl.when(iq == 0)
    def _():
        gap_s[...] = _gap(small, cols, bq)
        dk_s[...] = jnp.zeros_like(dk_s)
        dv_s[...] = jnp.zeros_like(dv_s)

        def prepare(n, _):
            rows = pl.ds(pl.multiple_of(n * chunk, chunk), chunk)
            cos, sin = cos_ref[rows, :], sin_ref[rows, :]
            for i in range(KV):
                at = slice(i * HEAD, (i + 1) * HEAD)
                k = _turn(k_ref[rows, at].astype(F32), cos, sin).astype(BF).astype(F32)
                k_s[i, rows, :] = k.astype(BF)
                kt_s[i, :, rows] = k.T.astype(BF)
                v_s[i, rows, :] = v_ref[rows, at]
            return _

        lax.fori_loop(0, tokens // chunk, prepare, None)

    mine = pl.ds(pl.multiple_of(iq * bq, bq), bq)
    cos, sin = cos_ref[mine, :], sin_ref[mine, :]
    for i in range(KV):
        for n in range(GROUP):
            at, rows = (i * GROUP + n) * HEAD, slice(n * bq, (n + 1) * bq)
            q_s[i, rows, :] = _turn(q_ref[:, at : at + HEAD].astype(F32), cos, sin).astype(BF)
            do = do_ref[:, at : at + HEAD]
            do_s[i, rows, :] = do
            both = do.astype(F32) * o_ref[:, at : at + HEAD].astype(F32)
            stat_s[2 * i : 2 * i + 1, rows] = lse_ref[i, n : n + 1, :] * LOG2E
            stat_s[2 * i + 1 : 2 * i + 2, rows] = both.T.sum(axis=0, keepdims=True)
    dq_s[...] = jnp.zeros_like(dq_s)

    def block(start, size, masked):
        here = pl.ds(pl.multiple_of(start, small), size)
        qs = [q_s[i, at : at + wide, :] for i, at in pieces]
        dos = [do_s[i, at : at + wide, :] for i, at in pieces]
        scores = [_dot(k_s[i, here, :], x, 1, 1) for (i, _), x in zip(pieces, qs)]
        dps = [_dot(v_s[i, here, :], x, 1, 1) for (i, _), x in zip(pieces, dos)]
        level = start - iq * bq
        for n, (i, at) in enumerate(pieces):
            p = jnp.exp2(scores[n] * e - stat_s[2 * i : 2 * i + 1, at : at + wide])
            if masked:
                p = jnp.where(gap_s[:, at : at + wide] >= level, p, 0.0)
            ds = (p * (dps[n] - stat_s[2 * i + 1 : 2 * i + 2, at : at + wide])).astype(BF)
            dv_s[i, here, :] += _dot(p.astype(BF), dos[n], 1, 0)
            dk_s[i, here, :] += _dot(ds, qs[n], 1, 0)
            dq_s[i, :, at : at + wide] += _dot(kt_s[i, :, here], ds, 1, 0)

    first = iq * bq
    lax.fori_loop(0, lax.div(first, big), lambda j, _: block(j * big, big, False), None)
    lax.fori_loop(lax.div(first, big) * (big // small), lax.div(first + bq + small - 1, small), lambda j, _: block(j * small, small, True), None)

    for i in range(KV):
        dq = (dq_s[i] * scale).T
        for n in range(GROUP):
            at = (i * GROUP + n) * HEAD
            d_ref[mine, at : at + HEAD] = _turn_back(dq[n * bq : (n + 1) * bq, :], cos, sin).astype(BF)

    @pl.when(iq == pl.num_programs(0) - 1)
    def _():
        def finish(n, _):
            rows = pl.ds(pl.multiple_of(n * chunk, chunk), chunk)
            cos, sin = cos_ref[rows, :], sin_ref[rows, :]
            for i in range(KV):
                at = QW + i * HEAD
                d_ref[rows, at : at + HEAD] = _turn_back(dk_s[i, rows, :] * scale, cos, sin).astype(BF)
                d_ref[rows, at + KW : at + KW + HEAD] = dv_s[i, rows, :].astype(BF)
            return _

        lax.fori_loop(0, tokens // chunk, finish, None)


def attend_back(qkv, o, do, lse, cos, sin, bq=128, wide=384, big=512, small=256):
    tokens = qkv.shape[0]
    cols = GROUP * bq
    rows = pl.BlockSpec((bq, QW), lambda i: (i, 0))
    return pl.pallas_call(
        functools.partial(_attend_back, bq=bq, wide=wide, big=big, small=small),
        grid=(tokens // bq,),
        in_specs=[rows, pl.BlockSpec((tokens, KW), lambda i: (0, QW // KW)), pl.BlockSpec((tokens, KW), lambda i: (0, QW // KW + 1)), rows, rows,
                  pl.BlockSpec((KV, GROUP, bq), lambda i: (0, 0, i)), _whole(tokens, HEAD), _whole(tokens, HEAD)],
        out_specs=_whole(tokens, QW + 2 * KW),
        out_shape=_shape(tokens, QW + 2 * KW),
        scratch_shapes=[pltpu.VMEM((KV, cols, HEAD), BF), pltpu.VMEM((KV, cols, HEAD), BF), pltpu.VMEM((KV, tokens, HEAD), BF),
                        pltpu.VMEM((KV, HEAD, tokens), BF), pltpu.VMEM((KV, tokens, HEAD), BF), pltpu.VMEM((KV, HEAD, cols), F32),
                        pltpu.VMEM((KV, tokens, HEAD), F32), pltpu.VMEM((KV, tokens, HEAD), F32), pltpu.VMEM((2 * KV, cols), F32),
                        pltpu.VMEM((small, cols), jnp.int32)],
        compiler_params=_params(),
        cost_estimate=_cost(5 * HEADS * tokens * tokens * HEAD, [qkv, qkv, o, do], HEADS * tokens * tokens // 2),
        name="attend_back",
    )(qkv, qkv, qkv, o, do, lse, cos, sin)


def _normed(h):
    wide = h.astype(F32)
    return (wide * lax.rsqrt(jnp.mean(wide**2, -1, keepdims=True) + 1e-6)).astype(BF)


def _plus(h, r):
    return (h.astype(F32) + r.astype(BF).astype(F32)).astype(BF)


def _norm_back(h, by_a, by_h):
    wide = h.astype(F32)
    by_a = by_a.astype(BF).astype(F32)
    scale = lax.rsqrt(jnp.mean(wide**2, -1, keepdims=True) + 1e-6)
    along = jnp.mean(wide * by_a, -1, keepdims=True)
    return (by_h.astype(F32) + scale * (by_a - wide * (scale * scale * along))).astype(BF)


def _rows(bt, width):
    return pl.BlockSpec((bt, width), lambda i: (i, 0))


def project(h, w, bt=512):
    def kernel(h_ref, w_ref, a_ref, out_ref):
        a = _normed(h_ref[...])
        a_ref[...] = a
        out_ref[...] = _dot(a, w_ref[...], 1, 0).astype(BF)

    (t, d), n = h.shape, w.shape[1]
    return pl.pallas_call(kernel, grid=(t // bt,), in_specs=[_rows(bt, d), _whole(d, n)], out_specs=[_rows(bt, d), _rows(bt, n)],
                          out_shape=[_shape(t, d), _shape(t, n)], compiler_params=_params(), cost_estimate=_cost(2 * t * d * n, [h, h, w]),
                          name="project")(h, w)


def attention_out(o, w, h, bt=512):
    def kernel(o_ref, w_ref, h_ref, h2_ref, b_ref):
        h2 = _plus(h_ref[...], _dot(o_ref[...], w_ref[...], 1, 0))
        h2_ref[...] = h2
        b_ref[...] = _normed(h2)

    (t, n), d = o.shape, w.shape[1]
    return pl.pallas_call(kernel, grid=(t // bt,), in_specs=[_rows(bt, n), _whole(n, d), _rows(bt, d)], out_specs=[_rows(bt, d), _rows(bt, d)],
                          out_shape=[_shape(t, d), _shape(t, d)], compiler_params=_params(), cost_estimate=_cost(2 * t * d * n, [h, h, w, o]),
                          name="attention_out")(o, w, h)


def mlp_in(b, w, nt=256, bt=512):
    def kernel(b_ref, g_ref, u_ref, act_ref, gate_ref, up_ref):
        for at in range(0, b_ref.shape[0], bt):
            here = slice(at, at + bt)
            gate = _dot(b_ref[here, :], g_ref[...], 1, 0)
            up = _dot(b_ref[here, :], u_ref[...], 1, 0)
            gate_ref[here, :] = gate
            up_ref[here, :] = up
            act_ref[here, :] = (gate * jax.nn.sigmoid(gate) * up).astype(BF)

    (t, d), f = b.shape, w.shape[1] // 2
    cols = lambda first: pl.BlockSpec((d, nt), lambda i: (0, first // nt + i))
    out = pl.BlockSpec((t, nt), lambda i: (0, i))
    return pl.pallas_call(kernel, grid=(f // nt,), in_specs=[_whole(t, d), cols(0), cols(f)], out_specs=[out] * 3,
                          out_shape=[_shape(t, f), _shape(t, f, dtype=F32), _shape(t, f, dtype=F32)], compiler_params=_params(),
                          cost_estimate=_cost(4 * t * d * f, [b, w]), name="mlp_in")(b, w, w)


def mlp_out(act, w, h, bt=512):
    def kernel(act_ref, w_ref, h_ref, out_ref):
        out_ref[...] = _plus(h_ref[...], _dot(act_ref[...], w_ref[...], 1, 0))

    (t, f), d = act.shape, w.shape[1]
    return pl.pallas_call(kernel, grid=(t // bt,), in_specs=[_rows(bt, f), _whole(f, d), _rows(bt, d)], out_specs=_rows(bt, d),
                          out_shape=_shape(t, d), compiler_params=_params(), cost_estimate=_cost(2 * t * d * f, [h, h, w, act]),
                          name="mlp_out")(act, w, h)


def _silu_back(gate, up, by_act):
    by_act = by_act.astype(BF).astype(F32)
    s = jax.nn.sigmoid(gate)
    return (by_act * up * (s * (1 + gate * (1 - s)))).astype(BF), (by_act * (gate * s)).astype(BF)


def mlp_turn(b, w, w_down, by_h, nt=256, bt=512):
    def kernel(b_ref, g_ref, u_ref, d_ref, by_ref, act_ref, by_gu_ref):
        for at in range(0, b_ref.shape[0], bt):
            here = slice(at, at + bt)
            gate = _dot(b_ref[here, :], g_ref[...], 1, 0)
            up = _dot(b_ref[here, :], u_ref[...], 1, 0)
            by_act = _dot(by_ref[here, :], d_ref[...], 1, 1)
            act_ref[here, :] = (gate * jax.nn.sigmoid(gate) * up).astype(BF)
            by_gu_ref[0, here, :], by_gu_ref[1, here, :] = _silu_back(gate, up, by_act)

    (t, d), f = b.shape, w.shape[1] // 2
    cols = lambda first: pl.BlockSpec((d, nt), lambda i: (0, first // nt + i))
    return pl.pallas_call(kernel, grid=(f // nt,),
                          in_specs=[_whole(t, d), cols(0), cols(f), pl.BlockSpec((nt, d), lambda i: (i, 0)), _whole(t, d)],
                          out_specs=[pl.BlockSpec((t, nt), lambda i: (0, i)), pl.BlockSpec((2, t, nt), lambda i: (0, 0, i))],
                          out_shape=[_shape(t, f), _shape(2, t, f)], compiler_params=_params(),
                          cost_estimate=_cost(6 * t * d * f, [b, w]), name="mlp_turn")(b, w, w, w_down, by_h)


def mlp_back(gate, up, w_down, by_h, nt=256, bt=512):
    def kernel(gate_ref, up_ref, d_ref, by_ref, by_gu_ref):
        for at in range(0, gate_ref.shape[0], bt):
            here = slice(at, at + bt)
            by_act = _dot(by_ref[here, :], d_ref[...], 1, 1)
            by_gu_ref[0, here, :], by_gu_ref[1, here, :] = _silu_back(gate_ref[here, :], up_ref[here, :], by_act)

    (t, f), d = gate.shape, by_h.shape[1]
    tile = pl.BlockSpec((t, nt), lambda i: (0, i))
    return pl.pallas_call(kernel, grid=(f // nt,), in_specs=[tile, tile, pl.BlockSpec((nt, d), lambda i: (i, 0)), _whole(t, d)],
                          out_specs=pl.BlockSpec((2, t, nt), lambda i: (0, 0, i)), out_shape=_shape(2, t, f), compiler_params=_params(),
                          cost_estimate=_cost(2 * t * d * f, [gate, up]), name="mlp_back")(gate, up, w_down, by_h)


def back_in_mlp(by_gu, w, h, by_h, bt=512):
    def kernel(by_ref, w_ref, h_ref, by_h_ref, out_ref):
        f = by_ref.shape[2]
        by_b = _dot(by_ref[0], w_ref[:, :f], 1, 1) + _dot(by_ref[1], w_ref[:, f:], 1, 1)
        out_ref[...] = _norm_back(h_ref[...], by_b, by_h_ref[...])

    (_, t, f), d = by_gu.shape, h.shape[1]
    return pl.pallas_call(kernel, grid=(t // bt,),
                          in_specs=[pl.BlockSpec((2, bt, f), lambda i: (0, i, 0)), _whole(d, 2 * f, once=True), _rows(bt, d), _rows(bt, d)],
                          out_specs=_rows(bt, d), out_shape=_shape(t, d), compiler_params=_params(),
                          cost_estimate=_cost(4 * t * d * f, [by_gu, w, h, h]), name="back_in_mlp")(by_gu, w, h, by_h)


def back_in_attention(by_qkv, w, h, by_h, bt=512):
    def kernel(by_ref, w_ref, h_ref, by_h_ref, out_ref):
        out_ref[...] = _norm_back(h_ref[...], _dot(by_ref[...], w_ref[...], 1, 1), by_h_ref[...])

    (t, n), d = by_qkv.shape, h.shape[1]
    return pl.pallas_call(kernel, grid=(t // bt,), in_specs=[_rows(bt, n), _whole(d, n), _rows(bt, d), _rows(bt, d)], out_specs=_rows(bt, d),
                          out_shape=_shape(t, d), compiler_params=_params(), cost_estimate=_cost(2 * t * d * n, [by_qkv, w, h, h]),
                          name="back_in_attention")(by_qkv, w, h, by_h)


def back_out(by_h, w, bt=512):
    def kernel(by_ref, w_ref, out_ref):
        out_ref[...] = _dot(by_ref[...], w_ref[...], 1, 1).astype(BF)

    (t, d), n = by_h.shape, w.shape[0]
    return pl.pallas_call(kernel, grid=(t // bt,), in_specs=[_rows(bt, d), _whole(n, d)], out_specs=_rows(bt, n),
                          out_shape=_shape(t, n), compiler_params=_params(), cost_estimate=_cost(2 * t * d * n, [by_h, w]),
                          name="back_out")(by_h, w)


GU, DOWN, OUT = 8192, 4096, 1536


def _turned_once(x_ref, xt_s):
    @pl.when(pl.program_id(0) == 0)
    def _():
        step = 256
        for at in range(0, x_ref.shape[1], step):
            xt_s[at : at + step, :] = x_ref[:, at : at + step].T


def grad_in(x, by, width, nt=512):
    def kernel(x_ref, by_ref, out_ref, xt_s):
        _turned_once(x_ref, xt_s)
        out_ref[...] = _dot(xt_s[...], by_ref[0], 1, 0).astype(BF)

    (t, d), (parts, _, f) = x.shape, by.shape
    per = f // nt
    return pl.pallas_call(kernel, grid=(parts * per,),
                          in_specs=[_whole(t, d), pl.BlockSpec((1, t, nt), lambda i: (i // per, 0, i % per))],
                          out_specs=pl.BlockSpec((d, nt), lambda i: (0, i)), out_shape=_shape(d, width),
                          scratch_shapes=[pltpu.VMEM((d, t), BF)], compiler_params=_params(),
                          cost_estimate=_cost(2 * t * d * f * parts, [x, by, by]), name="grad_in")(x, by)


def grad_down(act, by_h, into):
    def kernel(act_ref, by_ref, _, out_ref):
        got = _dot(act_ref[...], by_ref[...], 0, 0).astype(BF)
        for j in range(4):
            out_ref[:, j * 1024 : (j + 1) * 1024] = got[j * 64 : (j + 1) * 64, :]

    (t, f), d = act.shape, by_h.shape[1]
    return pl.pallas_call(kernel, grid=(16,),
                          in_specs=[pl.BlockSpec((t, f // 16), lambda i: (0, i)), _whole(t, d), pl.BlockSpec(memory_space=pl.ANY)],
                          out_specs=pl.BlockSpec((64, DOWN), lambda i: (i, GU // DOWN)), out_shape=_shape(*into.shape),
                          input_output_aliases={2: 0}, compiler_params=_params(),
                          cost_estimate=_cost(2 * t * d * f, [act, by_h]), name="grad_down")(act, by_h, into)


def grad_out(o, by_h, into):
    def kernel(o_ref, by_ref, _, out_ref):
        got = _dot(o_ref[...], by_ref[...], 0, 0).astype(BF)
        for n in range(4):
            left, right = got[n * 96 : (n + 1) * 96, :512], got[n * 96 : (n + 1) * 96, 512:]
            here = slice(n * 64, (n + 1) * 64)
            out_ref[here, :512] = left[:64]
            out_ref[here, 512:1024] = jnp.concatenate([left[64:], right[:32]], 0)
            out_ref[here, 1024:] = right[32:]

    (t, n), d = o.shape, by_h.shape[1]
    return pl.pallas_call(kernel, grid=(4,), in_specs=[pl.BlockSpec((t, n // 4), lambda i: (0, i)), _whole(t, d), pl.BlockSpec(memory_space=pl.ANY)],
                          out_specs=pl.BlockSpec((256, OUT), lambda i: (i, (GU + DOWN) // OUT)), out_shape=_shape(*into.shape),
                          input_output_aliases={2: 0}, compiler_params=_params(),
                          cost_estimate=_cost(2 * t * d * n, [o, by_h]), name="grad_out")(o, by_h, into)


def unpack(got):
    down = got[:, GU : GU + DOWN].reshape(64, 4, 1024).transpose(1, 0, 2).reshape(256, 1024)
    parts = got[:, GU + DOWN :]
    both = jnp.concatenate([parts[:, :512], parts[:, 512:1024], parts[:, 1024:]], 0)
    return got[:, : GU // 2], got[:, GU // 2 : GU], down, jnp.concatenate([both[:96], both[96:]], 1)


def _pick(t, axis, at):
    return lax.dynamic_index_in_dim(t, at, axis, keepdims=True)


def _total(terms):
    return functools.reduce(lambda a, b: a + b, (t.astype(F32) for t in terms))


def scatter_by_pairs(grad):
    index = lax.axis_index("dp")
    bits = {axis: (index >> (3 - axis)) & 1 for axis in range(4)}

    def exchange(terms, axis):
        send = _total([_pick(t, axis, 1 - bits[axis]) for t in terms]).astype(BF)
        got = lax.ppermute(send, "dp", [(i, i ^ (1 << (3 - axis))) for i in range(16)])
        return [_pick(t, axis, bits[axis]) for t in terms] + [got]

    rows, width = grad.shape
    terms = exchange([grad.reshape(2, 2, 2, 2, rows // 16, width)], 3)
    edges = [0, 640, 1280, width]
    done = []
    lanes = [[t[..., edges[n] : edges[n + 1]] for t in terms] for n in range(3)]
    for stage in range(3):
        lanes = [exchange(lanes[n], (stage + n) % 3) for n in range(3)]
    for n in range(3):
        done.append(_total(lanes[n]).astype(BF).reshape(rows // 16, -1))
    return jnp.concatenate(done, 1)


def solution(mesh):
    def gathered(w):
        return lax.all_gather(w, "dp", axis=0, tiled=True)

    def step(x, dy, wq, wk, wv, wo, w_gate, w_up, w_down):
        layers = wq.shape[0]
        x, dy = x[0], dy[0]
        cos, sin = tables(x.shape[0])
        w = []
        for n in range(layers):
            w.append((gathered(jnp.concatenate([wq[n], wk[n], wv[n]], 1)), gathered(wo[n]), gathered(jnp.concatenate([w_gate[n], w_up[n]], 1)),
                      gathered(w_down[n])))
        h, kept = x, []
        for n in range(layers):
            w_qkv, w_o, w_gu, w_d = w[n]
            a, qkv = project(h, w_qkv)
            o, lse = attend(qkv, cos, sin)
            h2, b = attention_out(o, w_o, h)
            if n < layers - 1:
                act, gate, up = mlp_in(b, w_gu)
                kept.append((h, a, qkv, o, lse, h2, b, act, gate, up))
                h = mlp_out(act, w_d, h2)
            else:
                act, by_gu = mlp_turn(b, w_gu, w_d, dy)
                kept.append((h, a, qkv, o, lse, h2, b, act))
        by_h, mine = dy, [None] * layers
        for n in reversed(range(layers)):
            w_qkv, w_o, w_gu, w_d = w[n]
            h, a, qkv, o, lse, h2, b, act = kept[n][:8]
            if n < layers - 1:
                by_gu = mlp_back(*kept[n][8:], w_d, by_h)
            grads = grad_down(act, by_h, grad_in(b, by_gu, GU + DOWN + OUT))
            by_h2 = back_in_mlp(by_gu, w_gu, h2, by_h)
            grads = grad_out(o, by_h2, grads)
            grads, by_h2 = lax.optimization_barrier((grads, by_h2))
            big = lax.psum_scatter(grads, "dp", scatter_dimension=0, tiled=True)
            by_qkv = attend_back(qkv, o, back_out(by_h2, w_o), lse, cos, sin)
            grad = grad_in(a, by_qkv[None], QW + 2 * KW)
            grad, by_qkv = lax.optimization_barrier((grad, by_qkv))
            small = scatter_by_pairs(grad) if n == 0 else lax.psum_scatter(grad, "dp", scatter_dimension=0, tiled=True)
            by_h = back_in_attention(by_qkv, w_qkv, h, by_h2)
            mine[n] = (big, small)
        outs = []
        for big, small in mine:
            gate, up, down, out = unpack(big)
            outs.append((small[:, :QW], small[:, QW : QW + KW], small[:, QW + KW :], out, gate, up, down))
        return (by_h[None], *(jnp.stack([outs[n][i] for n in range(layers)]) for i in range(7)))

    states, cut = P(("rep", "dp"), None, None), P(None, "dp", None)
    return jax.shard_map(step, mesh=mesh, in_specs=(states, states) + (cut,) * 7, out_specs=(states,) + (P("rep", "dp", None),) * 7, check_vma=False)
```

```python
import functools

import jax
import jax.numpy as jnp
from jax import lax
from jax.experimental import pallas as pl
from jax.experimental.pallas import tpu as pltpu
from jax.sharding import PartitionSpec as P

NEG = -1e30
HIDDEN = 2 * NEG
LOG2E = 1.4426950408889634
HEAD = 128
SHARD = 64
MODEL = 1024
HEADS = 12
KV = 2
GROUP = HEADS // KV
QW = HEADS * HEAD
KW = KV * HEAD
THETA = 10000
BF = jnp.bfloat16
F32 = jnp.float32
NAMES = ("wq", "wk", "wv", "wo", "w_gate", "w_up", "w_down")


def _dot(a, b, ca, cb):
    return lax.dot_general(a, b, (((ca,), (cb,)), ((), ())), preferred_element_type=F32)


def _params(steps=1, mib=60):
    return pltpu.CompilerParams(dimension_semantics=("arbitrary",) * steps, vmem_limit_bytes=mib * 2**20)


def _cost(flops, arrays, exps=0):
    return pl.CostEstimate(flops=int(flops), transcendentals=int(exps), bytes_accessed=sum(a.size * a.dtype.itemsize for a in arrays))


def _whole(*shape, once=False):
    mode = dict(pipeline_mode=pl.Buffered(1)) if once else {}
    return pl.BlockSpec(shape, lambda *_: (0,) * len(shape), **mode)


def _shape(*shape, dtype=BF):
    return jax.ShapeDtypeStruct(shape, dtype)


def _turn(t, cos, sin):
    return t * cos + pltpu.roll(t, HEAD // 2, 1) * sin


def _turn_back(t, cos, sin):
    return t * cos - pltpu.roll(t, HEAD // 2, 1) * sin


def tables(tokens):
    half = HEAD // 2
    angle = jnp.arange(tokens, dtype=F32)[:, None] * THETA ** (-jnp.arange(half, dtype=F32) / half)
    cos, sin = jnp.cos(angle), jnp.sin(angle)
    return jnp.concatenate([cos, cos], 1), jnp.concatenate([-sin, sin], 1)


def _gap(bk, cols, bq):
    return lax.rem(lax.broadcasted_iota(jnp.int32, (bk, cols), 1), bq) - lax.broadcasted_iota(jnp.int32, (bk, cols), 0)


def _attend(q_ref, k_ref, v_ref, cos_ref, sin_ref, o_ref, lse_ref, q_s, k_s, v_s, top_s, mix_s, gap_s, *, bq, wide, big, small):
    tokens = k_ref.shape[0]
    cols = GROUP * bq
    iq = pl.program_id(0)
    scale = HEAD**-0.5
    e = scale * LOG2E
    pieces = [(i, at) for i in range(KV) for at in range(0, cols, wide)]

    @pl.when(iq == 0)
    def _():
        gap_s[...] = _gap(small, cols, bq)
        chunk = 256

        def prepare(n, _):
            rows = pl.ds(pl.multiple_of(n * chunk, chunk), chunk)
            cos, sin = cos_ref[rows, :], sin_ref[rows, :]
            for i in range(KV):
                at = slice(i * HEAD, (i + 1) * HEAD)
                k_s[i, rows, :] = _turn(k_ref[rows, at].astype(F32), cos, sin).astype(BF)
                v_s[i, :HEAD, rows] = v_ref[rows, at].astype(F32).T.astype(BF)
                v_s[i, HEAD:, rows] = jnp.ones((16, chunk), BF)
            return _

        lax.fori_loop(0, tokens // chunk, prepare, None)

    mine = pl.ds(pl.multiple_of(iq * bq, bq), bq)
    cos, sin = cos_ref[mine, :], sin_ref[mine, :]
    for i in range(KV):
        for n in range(GROUP):
            at = (i * GROUP + n) * HEAD
            q_s[i, n * bq : (n + 1) * bq, :] = _turn(q_ref[:, at : at + HEAD].astype(F32), cos, sin).astype(BF)
    top_s[...] = jnp.full(top_s.shape, NEG, F32)
    mix_s[...] = jnp.zeros(mix_s.shape, F32)

    def block(start, size, masked):
        here = pl.ds(pl.multiple_of(start, small), size)
        scores = [_dot(k_s[i, here, :], q_s[i, at : at + wide, :], 1, 1) for i, at in pieces]
        weights, keeps = [], []
        level = start - iq * bq
        for (i, at), s in zip(pieces, scores):
            if masked:
                s = jnp.where(gap_s[:, at : at + wide] >= level, s, HIDDEN)
            old = top_s[i : i + 1, at : at + wide]
            top = jnp.maximum(old, s.max(axis=0, keepdims=True))
            top_s[i : i + 1, at : at + wide] = top
            weights.append(jnp.exp2((s - top) * e).astype(BF))
            keeps.append(jnp.exp2((old - top) * e))
        for (i, at), p, keep in zip(pieces, weights, keeps):
            mix_s[i, :, at : at + wide] = mix_s[i, :, at : at + wide] * keep + _dot(v_s[i, :, here], p, 1, 0)

    first = iq * bq
    lax.fori_loop(0, lax.div(first, big), lambda j, _: block(j * big, big, False), None)
    lax.fori_loop(lax.div(first, big) * (big // small), lax.div(first + bq + small - 1, small), lambda j, _: block(j * small, small, True), None)

    for i in range(KV):
        top, total = top_s[i : i + 1, :], mix_s[i, HEAD : HEAD + 1, :]
        out = (mix_s[i, :HEAD, :] * (1 / total)).T
        lse = top * scale + jnp.log(total)
        for n in range(GROUP):
            at = (i * GROUP + n) * HEAD
            o_ref[:, at : at + HEAD] = out[n * bq : (n + 1) * bq, :].astype(BF)
            lse_ref[i, n : n + 1, :] = lse[:, n * bq : (n + 1) * bq]


def attend(qkv, cos, sin, bq=256, wide=512, big=512, small=256):
    tokens = qkv.shape[0]
    cols = GROUP * bq
    return pl.pallas_call(
        functools.partial(_attend, bq=bq, wide=wide, big=big, small=small),
        grid=(tokens // bq,),
        in_specs=[pl.BlockSpec((bq, QW), lambda i: (i, 0)), pl.BlockSpec((tokens, KW), lambda i: (0, QW // KW)),
                  pl.BlockSpec((tokens, KW), lambda i: (0, QW // KW + 1)), _whole(tokens, HEAD), _whole(tokens, HEAD)],
        out_specs=[pl.BlockSpec((bq, QW), lambda i: (i, 0)), pl.BlockSpec((KV, GROUP, bq), lambda i: (0, 0, i))],
        out_shape=[_shape(tokens, QW), _shape(KV, GROUP, tokens, dtype=F32)],
        scratch_shapes=[pltpu.VMEM((KV, cols, HEAD), BF), pltpu.VMEM((KV, tokens, HEAD), BF), pltpu.VMEM((KV, HEAD + 16, tokens), BF),
                        pltpu.VMEM((KV, cols), F32), pltpu.VMEM((KV, HEAD + 16, cols), F32), pltpu.VMEM((small, cols), jnp.int32)],
        compiler_params=_params(),
        cost_estimate=_cost(2 * HEADS * tokens * tokens * HEAD, [qkv, qkv], HEADS * tokens * tokens // 2),
        name="attend",
    )(qkv, qkv, qkv, cos, sin)


def _attend_back(q_ref, k_ref, v_ref, o_ref, do_ref, lse_ref, cos_ref, sin_ref, d_ref, q_s, do_s, k_s, kt_s, v_s, dq_s, dk_s, dv_s, stat_s, gap_s,
                 *, bq, wide, big, small):
    tokens = k_ref.shape[0]
    cols = GROUP * bq
    iq = pl.program_id(0)
    scale = HEAD**-0.5
    e = scale * LOG2E
    pieces = [(i, at) for i in range(KV) for at in range(0, cols, wide)]
    chunk = 256

    @pl.when(iq == 0)
    def _():
        gap_s[...] = _gap(small, cols, bq)
        dk_s[...] = jnp.zeros_like(dk_s)
        dv_s[...] = jnp.zeros_like(dv_s)

        def prepare(n, _):
            rows = pl.ds(pl.multiple_of(n * chunk, chunk), chunk)
            cos, sin = cos_ref[rows, :], sin_ref[rows, :]
            for i in range(KV):
                at = slice(i * HEAD, (i + 1) * HEAD)
                k = _turn(k_ref[rows, at].astype(F32), cos, sin).astype(BF).astype(F32)
                k_s[i, rows, :] = k.astype(BF)
                kt_s[i, :, rows] = k.T.astype(BF)
                v_s[i, rows, :] = v_ref[rows, at]
            return _

        lax.fori_loop(0, tokens // chunk, prepare, None)

    mine = pl.ds(pl.multiple_of(iq * bq, bq), bq)
    cos, sin = cos_ref[mine, :], sin_ref[mine, :]
    for i in range(KV):
        for n in range(GROUP):
            at, rows = (i * GROUP + n) * HEAD, slice(n * bq, (n + 1) * bq)
            q_s[i, rows, :] = _turn(q_ref[:, at : at + HEAD].astype(F32), cos, sin).astype(BF)
            do = do_ref[:, at : at + HEAD]
            do_s[i, rows, :] = do
            both = do.astype(F32) * o_ref[:, at : at + HEAD].astype(F32)
            stat_s[2 * i : 2 * i + 1, rows] = lse_ref[i, n : n + 1, :] * LOG2E
            stat_s[2 * i + 1 : 2 * i + 2, rows] = both.T.sum(axis=0, keepdims=True)
    dq_s[...] = jnp.zeros_like(dq_s)

    def block(start, size, masked):
        here = pl.ds(pl.multiple_of(start, small), size)
        qs = [q_s[i, at : at + wide, :] for i, at in pieces]
        dos = [do_s[i, at : at + wide, :] for i, at in pieces]
        scores = [_dot(k_s[i, here, :], x, 1, 1) for (i, _), x in zip(pieces, qs)]
        dps = [_dot(v_s[i, here, :], x, 1, 1) for (i, _), x in zip(pieces, dos)]
        level = start - iq * bq
        for n, (i, at) in enumerate(pieces):
            p = jnp.exp2(scores[n] * e - stat_s[2 * i : 2 * i + 1, at : at + wide])
            if masked:
                p = jnp.where(gap_s[:, at : at + wide] >= level, p, 0.0)
            ds = (p * (dps[n] - stat_s[2 * i + 1 : 2 * i + 2, at : at + wide])).astype(BF)
            dv_s[i, here, :] += _dot(p.astype(BF), dos[n], 1, 0)
            dk_s[i, here, :] += _dot(ds, qs[n], 1, 0)
            dq_s[i, :, at : at + wide] += _dot(kt_s[i, :, here], ds, 1, 0)

    first = iq * bq
    lax.fori_loop(0, lax.div(first, big), lambda j, _: block(j * big, big, False), None)
    lax.fori_loop(lax.div(first, big) * (big // small), lax.div(first + bq + small - 1, small), lambda j, _: block(j * small, small, True), None)

    for i in range(KV):
        dq = (dq_s[i] * scale).T
        for n in range(GROUP):
            at = (i * GROUP + n) * HEAD
            d_ref[mine, at : at + HEAD] = _turn_back(dq[n * bq : (n + 1) * bq, :], cos, sin).astype(BF)

    @pl.when(iq == pl.num_programs(0) - 1)
    def _():
        def finish(n, _):
            rows = pl.ds(pl.multiple_of(n * chunk, chunk), chunk)
            cos, sin = cos_ref[rows, :], sin_ref[rows, :]
            for i in range(KV):
                at = QW + i * HEAD
                d_ref[rows, at : at + HEAD] = _turn_back(dk_s[i, rows, :] * scale, cos, sin).astype(BF)
                d_ref[rows, at + KW : at + KW + HEAD] = dv_s[i, rows, :].astype(BF)
            return _

        lax.fori_loop(0, tokens // chunk, finish, None)


def attend_back(qkv, o, do, lse, cos, sin, bq=256, wide=512, big=512, small=256):
    tokens = qkv.shape[0]
    cols = GROUP * bq
    rows = pl.BlockSpec((bq, QW), lambda i: (i, 0))
    return pl.pallas_call(
        functools.partial(_attend_back, bq=bq, wide=wide, big=big, small=small),
        grid=(tokens // bq,),
        in_specs=[rows, pl.BlockSpec((tokens, KW), lambda i: (0, QW // KW)), pl.BlockSpec((tokens, KW), lambda i: (0, QW // KW + 1)), rows, rows,
                  pl.BlockSpec((KV, GROUP, bq), lambda i: (0, 0, i)), _whole(tokens, HEAD), _whole(tokens, HEAD)],
        out_specs=_whole(tokens, QW + 2 * KW),
        out_shape=_shape(tokens, QW + 2 * KW),
        scratch_shapes=[pltpu.VMEM((KV, cols, HEAD), BF), pltpu.VMEM((KV, cols, HEAD), BF), pltpu.VMEM((KV, tokens, HEAD), BF),
                        pltpu.VMEM((KV, HEAD, tokens), BF), pltpu.VMEM((KV, tokens, HEAD), BF), pltpu.VMEM((KV, HEAD, cols), F32),
                        pltpu.VMEM((KV, tokens, HEAD), F32), pltpu.VMEM((KV, tokens, HEAD), F32), pltpu.VMEM((2 * KV, cols), F32),
                        pltpu.VMEM((small, cols), jnp.int32)],
        compiler_params=_params(),
        cost_estimate=_cost(5 * HEADS * tokens * tokens * HEAD, [qkv, qkv, o, do], HEADS * tokens * tokens // 2),
        name="attend_back",
    )(qkv, qkv, qkv, o, do, lse, cos, sin)


def _normed(h):
    wide = h.astype(F32)
    return (wide * lax.rsqrt(jnp.mean(wide**2, -1, keepdims=True) + 1e-6)).astype(BF)


def _plus(h, r):
    return (h.astype(F32) + r.astype(BF).astype(F32)).astype(BF)


def _norm_back(h, by_a, by_h):
    wide = h.astype(F32)
    by_a = by_a.astype(BF).astype(F32)
    scale = lax.rsqrt(jnp.mean(wide**2, -1, keepdims=True) + 1e-6)
    along = jnp.mean(wide * by_a, -1, keepdims=True)
    return (by_h.astype(F32) + scale * (by_a - wide * (scale * scale * along))).astype(BF)


def _rows(bt, width):
    return pl.BlockSpec((bt, width), lambda i: (i, 0))


class Part:
    def __init__(self, array, first, width):
        self.array, self.first, self.width = array, first, width

    def spec(self, rows, width, index):
        base = self.first // width

        def at(*ids):
            r, c = index(*ids)
            return r, base + c

        return pl.BlockSpec((rows, width), at)


def _o_specs(w):
    return [w.spec(MODEL, 512, lambda *_, n=n: (0, n)) for n in range(3)]


def _o_whole(refs, w_s):
    @pl.when(pl.program_id(0) == 0)
    def _():
        one, two, three = refs
        for n in range(16):
            w_s[n * 96 : n * 96 + SHARD, :512] = one[n * SHARD : (n + 1) * SHARD, :]
            w_s[n * 96 + SHARD : (n + 1) * 96, :512] = two[n * SHARD : n * SHARD + 32, :]
            w_s[n * 96 : n * 96 + 32, 512:] = two[n * SHARD + 32 : (n + 1) * SHARD, :]
            w_s[n * 96 + 32 : (n + 1) * 96, 512:] = three[n * SHARD : (n + 1) * SHARD, :]


def _down_tile(ref):
    return jnp.concatenate([ref[:, j * MODEL : (j + 1) * MODEL] for j in range(4)], 0)


def project(h, w, bt=512, sub=256):
    def kernel(h_ref, w_ref, a_ref, out_ref):
        for at in range(0, bt, sub):
            here = slice(at, at + sub)
            a = _normed(h_ref[here, :])
            a_ref[here, :] = a
            out_ref[here, :] = _dot(a, w_ref[...], 1, 0).astype(BF)

    (t, d), n = h.shape, w.width
    return pl.pallas_call(kernel, grid=(t // bt,), in_specs=[_rows(bt, d), w.spec(d, n, lambda i: (0, 0))], out_specs=[_rows(bt, d), _rows(bt, n)],
                          out_shape=[_shape(t, d), _shape(t, n)], compiler_params=_params(), cost_estimate=_cost(2 * t * d * n, [h, h]),
                          name="project")(h, w.array)


def attention_out(o, w, h, bt=512, sub=256):
    def kernel(o_ref, w0, w1, w2, h_ref, h2_ref, b_ref, w_s):
        _o_whole((w0, w1, w2), w_s)
        for at in range(0, bt, sub):
            here = slice(at, at + sub)
            h2 = _plus(h_ref[here, :], _dot(o_ref[here, :], w_s[...], 1, 0))
            h2_ref[here, :] = h2
            b_ref[here, :] = _normed(h2)

    (t, n), d = o.shape, h.shape[1]
    return pl.pallas_call(kernel, grid=(t // bt,), in_specs=[_rows(bt, n), *_o_specs(w), _rows(bt, d)], out_specs=[_rows(bt, d), _rows(bt, d)],
                          out_shape=[_shape(t, d), _shape(t, d)], scratch_shapes=[pltpu.VMEM((n, d), BF)], compiler_params=_params(),
                          cost_estimate=_cost(2 * t * d * n, [h, h, o]), name="attention_out")(o, *[w.array] * 3, h)


def back_out(by_h, w, bt=512):
    def kernel(by_ref, w0, w1, w2, out_ref, w_s):
        _o_whole((w0, w1, w2), w_s)
        out_ref[...] = _dot(by_ref[...], w_s[...], 1, 1).astype(BF)

    (t, d), n = by_h.shape, QW
    return pl.pallas_call(kernel, grid=(t // bt,), in_specs=[_rows(bt, d), *_o_specs(w)], out_specs=_rows(bt, n), out_shape=_shape(t, n),
                          scratch_shapes=[pltpu.VMEM((n, d), BF)], compiler_params=_params(), cost_estimate=_cost(2 * t * d * n, [by_h]),
                          name="back_out")(by_h, *[w.array] * 3)


def mlp_in(b, w, nt=256, bt=512):
    def kernel(b_ref, g_ref, u_ref, act_ref, gate_ref, up_ref):
        for at in range(0, b_ref.shape[0], bt):
            here = slice(at, at + bt)
            gate = _dot(b_ref[here, :], g_ref[...], 1, 0)
            up = _dot(b_ref[here, :], u_ref[...], 1, 0)
            gate_ref[here, :] = gate
            up_ref[here, :] = up
            act_ref[here, :] = (gate * jax.nn.sigmoid(gate) * up).astype(BF)

    (t, d), f = b.shape, w.width // 2
    out = pl.BlockSpec((t, nt), lambda i: (0, i))
    return pl.pallas_call(kernel, grid=(f // nt,),
                          in_specs=[_whole(t, d), w.spec(d, nt, lambda i: (0, i)), w.spec(d, nt, lambda i: (0, f // nt + i))], out_specs=[out] * 3,
                          out_shape=[_shape(t, f), _shape(t, f, dtype=F32), _shape(t, f, dtype=F32)], compiler_params=_params(),
                          cost_estimate=_cost(4 * t * d * f, [b]), name="mlp_in")(b, w.array, w.array)


def mlp_out(act, w, h, bt=512):
    def kernel(act_ref, w_ref, h_ref, out_ref, w_s):
        @pl.when(pl.program_id(0) == 0)
        def _():
            for n in range(16):
                for j in range(4):
                    w_s[n * 256 + j * SHARD : n * 256 + (j + 1) * SHARD, :] = w_ref[n * SHARD : (n + 1) * SHARD, j * MODEL : (j + 1) * MODEL]

        out_ref[...] = _plus(h_ref[...], _dot(act_ref[...], w_s[...], 1, 0))

    (t, f), d = act.shape, h.shape[1]
    return pl.pallas_call(kernel, grid=(t // bt,), in_specs=[_rows(bt, f), w.spec(MODEL, DOWN, lambda i: (0, 0)), _rows(bt, d)], out_specs=_rows(bt, d),
                          out_shape=_shape(t, d), scratch_shapes=[pltpu.VMEM((f, d), BF)], compiler_params=_params(),
                          cost_estimate=_cost(2 * t * d * f, [h, h, act]), name="mlp_out")(act, w.array, h)


def _silu_back(gate, up, by_act):
    by_act = by_act.astype(BF).astype(F32)
    s = jax.nn.sigmoid(gate)
    return (by_act * up * (s * (1 + gate * (1 - s)))).astype(BF), (by_act * (gate * s)).astype(BF)


def mlp_turn(b, w, w_down, by_h, nt=256, bt=512):
    def kernel(b_ref, g_ref, u_ref, d_ref, by_ref, act_ref, by_gu_ref):
        down = _down_tile(d_ref)
        for at in range(0, b_ref.shape[0], bt):
            here = slice(at, at + bt)
            gate = _dot(b_ref[here, :], g_ref[...], 1, 0)
            up = _dot(b_ref[here, :], u_ref[...], 1, 0)
            by_act = _dot(by_ref[here, :], down, 1, 1)
            act_ref[here, :] = (gate * jax.nn.sigmoid(gate) * up).astype(BF)
            by_gu_ref[0, here, :], by_gu_ref[1, here, :] = _silu_back(gate, up, by_act)

    (t, d), f = b.shape, w.width // 2
    return pl.pallas_call(kernel, grid=(f // nt,),
                          in_specs=[_whole(t, d), w.spec(d, nt, lambda i: (0, i)), w.spec(d, nt, lambda i: (0, f // nt + i)),
                                    w_down.spec(SHARD, DOWN, lambda i: (i, 0)), _whole(t, d)],
                          out_specs=[pl.BlockSpec((t, nt), lambda i: (0, i)), pl.BlockSpec((2, t, nt), lambda i: (0, 0, i))],
                          out_shape=[_shape(t, f), _shape(2, t, f)], compiler_params=_params(),
                          cost_estimate=_cost(6 * t * d * f, [b]), name="mlp_turn")(b, w.array, w.array, w_down.array, by_h)


def mlp_back(gate, up, w_down, by_h, nt=256, bt=512):
    def kernel(gate_ref, up_ref, d_ref, by_ref, by_gu_ref):
        down = _down_tile(d_ref)
        for at in range(0, gate_ref.shape[0], bt):
            here = slice(at, at + bt)
            by_act = _dot(by_ref[here, :], down, 1, 1)
            by_gu_ref[0, here, :], by_gu_ref[1, here, :] = _silu_back(gate_ref[here, :], up_ref[here, :], by_act)

    (t, f), d = gate.shape, by_h.shape[1]
    tile = pl.BlockSpec((t, nt), lambda i: (0, i))
    return pl.pallas_call(kernel, grid=(f // nt,), in_specs=[tile, tile, w_down.spec(SHARD, DOWN, lambda i: (i, 0)), _whole(t, d)],
                          out_specs=pl.BlockSpec((2, t, nt), lambda i: (0, 0, i)), out_shape=_shape(2, t, f), compiler_params=_params(),
                          cost_estimate=_cost(2 * t * d * f, [gate, up]), name="mlp_back")(gate, up, w_down.array, by_h)


def back_in_mlp(by_gu, w, h, by_h, bt=512):
    def kernel(by_ref, w_ref, h_ref, by_h_ref, out_ref):
        f = by_ref.shape[2]
        by_b = _dot(by_ref[0], w_ref[:, :f], 1, 1) + _dot(by_ref[1], w_ref[:, f:], 1, 1)
        out_ref[...] = _norm_back(h_ref[...], by_b, by_h_ref[...])

    (_, t, f), d = by_gu.shape, h.shape[1]
    return pl.pallas_call(kernel, grid=(t // bt,),
                          in_specs=[pl.BlockSpec((2, bt, f), lambda i: (0, i, 0)), _whole(d, 2 * f, once=True), _rows(bt, d), _rows(bt, d)],
                          out_specs=_rows(bt, d), out_shape=_shape(t, d), compiler_params=_params(),
                          cost_estimate=_cost(4 * t * d * f, [by_gu, h, h]), name="back_in_mlp")(by_gu, w.array, h, by_h)


def back_in_attention(by_qkv, w, h, by_h, bt=512, sub=256):
    def kernel(by_ref, w_ref, h_ref, by_h_ref, out_ref):
        for at in range(0, bt, sub):
            here = slice(at, at + sub)
            out_ref[here, :] = _norm_back(h_ref[here, :], _dot(by_ref[here, :], w_ref[...], 1, 1), by_h_ref[here, :])

    (t, n), d = by_qkv.shape, h.shape[1]
    return pl.pallas_call(kernel, grid=(t // bt,), in_specs=[_rows(bt, n), w.spec(d, n, lambda i: (0, 0)), _rows(bt, d), _rows(bt, d)],
                          out_specs=_rows(bt, d), out_shape=_shape(t, d), compiler_params=_params(),
                          cost_estimate=_cost(2 * t * d * n, [by_qkv, h, h]), name="back_in_attention")(by_qkv, w.array, h, by_h)


GU, DOWN, OUT = 8192, 4096, 1536
WIDTH = GU + DOWN + OUT
PAD = 256


def _turned_once(x_ref, xt_s):
    @pl.when(pl.program_id(0) == 0)
    def _():
        step = 256
        for at in range(0, x_ref.shape[1], step):
            xt_s[at : at + step, :] = x_ref[:, at : at + step].T


def grad_in(x, by, width=None, into=None, first=0, nt=512):
    def kernel(x_ref, by_ref, *rest):
        out_ref, xt_s = rest[-2:]
        _turned_once(x_ref, xt_s)
        out_ref[...] = _dot(xt_s[...], by_ref[0], 1, 0).astype(BF)

    (t, d), (parts, _, f) = x.shape, by.shape
    per = f // nt
    more = [] if into is None else [into]
    return pl.pallas_call(kernel, grid=(parts * per,),
                          in_specs=[_whole(t, d), pl.BlockSpec((1, t, nt), lambda i: (i // per, 0, i % per))] + [pl.BlockSpec(memory_space=pl.ANY)] * len(more),
                          out_specs=pl.BlockSpec((d, nt), lambda i: (0, first // nt + i)), out_shape=_shape(d, width or into.shape[1]),
                          scratch_shapes=[pltpu.VMEM((d, t), BF)], compiler_params=_params(), input_output_aliases={2: 0} if more else {},
                          cost_estimate=_cost(2 * t * d * f * parts, [x, by, by]), name="grad_in")(x, by, *more)


def grad_down(act, by_h, into):
    def kernel(act_ref, by_ref, _, out_ref):
        got = _dot(act_ref[...], by_ref[...], 0, 0).astype(BF)
        for j in range(4):
            out_ref[:, j * MODEL : (j + 1) * MODEL] = got[j * SHARD : (j + 1) * SHARD, :]

    (t, f), d = act.shape, by_h.shape[1]
    return pl.pallas_call(kernel, grid=(16,),
                          in_specs=[pl.BlockSpec((t, f // 16), lambda i: (0, i)), _whole(t, d), pl.BlockSpec(memory_space=pl.ANY)],
                          out_specs=pl.BlockSpec((SHARD, DOWN), lambda i: (i, GU // DOWN)), out_shape=_shape(*into.shape),
                          input_output_aliases={2: 0}, compiler_params=_params(),
                          cost_estimate=_cost(2 * t * d * f, [act, by_h]), name="grad_down")(act, by_h, into)


def grad_out(o, by_h, into):
    def kernel(o_ref, by_ref, _, out_ref):
        got = _dot(o_ref[...], by_ref[...], 0, 0).astype(BF)
        for n in range(4):
            left, right = got[n * 96 : (n + 1) * 96, :512], got[n * 96 : (n + 1) * 96, 512:]
            here = slice(n * SHARD, (n + 1) * SHARD)
            out_ref[here, :512] = left[:SHARD]
            out_ref[here, 512:MODEL] = jnp.concatenate([left[SHARD:], right[:32]], 0)
            out_ref[here, MODEL:] = right[32:]

    (t, n), d = o.shape, by_h.shape[1]
    return pl.pallas_call(kernel, grid=(4,), in_specs=[pl.BlockSpec((t, n // 4), lambda i: (0, i)), _whole(t, d), pl.BlockSpec(memory_space=pl.ANY)],
                          out_specs=pl.BlockSpec((256, OUT), lambda i: (i, (GU + DOWN) // OUT)), out_shape=_shape(*into.shape),
                          input_output_aliases={2: 0}, compiler_params=_params(),
                          cost_estimate=_cost(2 * t * d * n, [o, by_h]), name="grad_out")(o, by_h, into)


def pack_o(w):
    both = jnp.concatenate([w[:, :512], w[:, 512:]], 0)
    return [both[n * SHARD : (n + 1) * SHARD] for n in range(3)]


def pack_down(w):
    return [w[n * SHARD : (n + 1) * SHARD] for n in range(4)]


def unpack(got):
    down = got[:, GU : GU + DOWN].reshape(SHARD, 4, MODEL).transpose(1, 0, 2).reshape(256, MODEL)
    parts = got[:, GU + DOWN : GU + DOWN + OUT]
    both = jnp.concatenate([parts[:, :512], parts[:, 512:MODEL], parts[:, MODEL:]], 0)
    return got[:, : GU // 2], got[:, GU // 2 : GU], down, jnp.concatenate([both[:96], both[96:]], 1)


def _pick(t, axis, at):
    return lax.dynamic_index_in_dim(t, at, axis, keepdims=True)


def _total(terms):
    return functools.reduce(lambda a, b: a + b, (t.astype(F32) for t in terms))


def scatter_by_pairs(grad):
    index = lax.axis_index("dp")
    bits = {axis: (index >> (3 - axis)) & 1 for axis in range(4)}

    def exchange(terms, axis):
        send = _total([_pick(t, axis, 1 - bits[axis]) for t in terms]).astype(BF)
        got = lax.ppermute(send, "dp", [(i, i ^ (1 << (3 - axis))) for i in range(16)])
        return [_pick(t, axis, bits[axis]) for t in terms] + [got]

    rows, width = grad.shape
    terms = exchange([grad.reshape(2, 2, 2, 2, rows // 16, width)], 3)
    edges = [0, 640, 1280, width]
    done = []
    lanes = [[t[..., edges[n] : edges[n + 1]] for t in terms] for n in range(3)]
    for stage in range(3):
        lanes = [exchange(lanes[n], (stage + n) % 3) for n in range(3)]
    for n in range(3):
        done.append(_total(lanes[n]).astype(BF).reshape(rows // 16, -1))
    return jnp.concatenate(done, 1)


def solution(mesh):
    def gathered(w):
        return lax.all_gather(w, "dp", axis=0, tiled=True)

    def step(x, dy, wq, wk, wv, wo, w_gate, w_up, w_down):
        x, dy = x[0], dy[0]
        cos, sin = tables(x.shape[0])
        qkv_w = QW + 2 * KW
        side = lambda parts: gathered(jnp.concatenate(parts, 1))
        qkv_of, gu_of = lambda n: [wq[n], wk[n], wv[n]], lambda n: [w_gate[n], w_up[n]]
        one = side(qkv_of(0))
        two = side(gu_of(0) + pack_o(wo[0]))
        three = side(pack_down(w_down[0]) + qkv_of(1) + pack_o(wo[1]))
        four = side(gu_of(1) + pack_down(w_down[1]))
        w = [(Part(one, 0, qkv_w), Part(two, GU, OUT), Part(two, 0, GU), Part(three, 0, DOWN)),
             (Part(three, DOWN, qkv_w), Part(three, DOWN + qkv_w, OUT), Part(four, 0, GU), Part(four, GU, DOWN))]

        h, kept = x, []
        for n, (w_qkv, w_o, w_gu, w_d) in enumerate(w):
            a, qkv = project(h, w_qkv)
            o, lse = attend(qkv, cos, sin)
            h2, b = attention_out(o, w_o, h)
            if n == 0:
                act, gate, up = mlp_in(b, w_gu)
                kept.append((h, a, qkv, o, lse, h2, b, act))
                h = mlp_out(act, w_d, h2)
            else:
                act, by_gu = mlp_turn(b, w_gu, w_d, dy)
                kept.append((h, a, qkv, o, lse, h2, b, act))

        by_h, mine = dy, [None, None]
        for n in (1, 0):
            w_qkv, w_o, w_gu, w_d = w[n]
            h, a, qkv, o, lse, h2, b, act = kept[n]
            if n == 0:
                by_gu = mlp_back(gate, up, w_d, by_h)
            grads = grad_down(act, by_h, grad_in(b, by_gu, width=WIDTH + n * (qkv_w + PAD)))
            by_h2 = back_in_mlp(by_gu, w_gu, h2, by_h)
            grads = grad_out(o, by_h2, grads)
            if n == 0:
                grads, by_h2, last = lax.optimization_barrier((grads, by_h2, mine[1][0]))
                mine[1] = (last, last[:, WIDTH : WIDTH + qkv_w])
                big = lax.psum_scatter(grads, "dp", scatter_dimension=0, tiled=True)
            by_qkv = attend_back(qkv, o, back_out(by_h2, w_o), lse, cos, sin)
            if n == 0:
                grad = grad_in(a, by_qkv[None], width=qkv_w)
                grad, by_qkv = lax.optimization_barrier((grad, by_qkv))
                small = scatter_by_pairs(grad)
            else:
                grads = grad_in(a, by_qkv[None], into=grads, first=WIDTH)
                grads, by_qkv = lax.optimization_barrier((grads, by_qkv))
                big = lax.psum_scatter(grads, "dp", scatter_dimension=0, tiled=True)
                small = None
            by_h = back_in_attention(by_qkv, w_qkv, h, by_h2)
            mine[n] = (big, small)
        outs = []
        for big, small in mine:
            gate, up, down, out = unpack(big)
            outs.append((small[:, :QW], small[:, QW : QW + KW], small[:, QW + KW :], out, gate, up, down))
        return (by_h[None], *(jnp.stack([outs[n][i] for n in range(2)]) for i in range(7)))

    states, cut = P(("rep", "dp"), None, None), P(None, "dp", None)
    return jax.shard_map(step, mesh=mesh, in_specs=(states, states) + (cut,) * 7, out_specs=(states,) + (P("rep", "dp", None),) * 7, check_vma=False)
```
